128 devices in a mesh: ta: 2 (over core), gx: 64 (over z, y, x).
Axes of the slice: x: 4, y: 4, z: 4, core: 2. Of those that a mesh axis runs over, the one named last changes fastest.
Arguments:
- time_links: float32 [6, 2, 3, 3, 384, 4608], P('ta', None, None, None, 'gx'), may hold values from -1 to 1, as said below
Outputs:
- loop_planes: float32 [384, 2, 4608], P('gx', None, 'ta')
- correlator: float32 [384, 193], P('gx')
The draws below stay inside these ranges and needn't reach their ends.
Inputs may be any that keep to these rules, and one draw needn't show every extreme that they name: At every site and time, the matrix time_links[t, 0] + i time_links[t, 1] is special unitary.
All inputs are finite; a program needn't handle non-finite values.
Results may differ from the reference program's by a relative error of at most 0.00029.
Values sent between devices are 32-bit elements; how exact they have to be, the bound alone decides.
No kernel may reach another device: no remote copies, remote signals or barrier semaphores. Data moves between devices by JAX's collectives and lax.ppermute only.
A program may use at most 64 MiB of HBM per device.

```python
import jax
import jax.numpy as jnp
from jax import lax

NY = 48
NZ = 96
NT = 6
NX = 384
RMAX = 192


def normalize(column_real, column_imag):
    inverse = lax.rsqrt(jnp.sum(column_real * column_real + column_imag * column_imag, axis=0) + 1e-20)
    return (column_real * inverse, column_imag * inverse)


def project(base_real, base_imag, column_real, column_imag):
    inner_real = jnp.sum(base_real * column_real + base_imag * column_imag, axis=0)
    inner_imag = jnp.sum(base_real * column_imag - base_imag * column_real, axis=0)
    new_real = column_real - (base_real * inner_real - base_imag * inner_imag)
    new_imag = column_imag - (base_real * inner_imag + base_imag * inner_real)
    return (new_real, new_imag)


def times_complex(first_real, first_imag, second_real, second_imag):
    return (first_real * second_real - first_imag * second_imag, first_real * second_imag + first_imag * second_real)


def along_planes(innovation, rate):
    keep = jnp.sqrt(1.0 - rate * rate)

    def advance(state, fresh):
        following = rate * state + keep * fresh
        return (following, following)
    first = innovation[0]
    _, rest = lax.scan(advance, first, innovation[1:])
    return jnp.concatenate([first[None], rest], axis=0)


def draw_time_links(key, part):
    base_key = jax.random.fold_in(key, 17)
    noise_key, scale_key, field_key, rate_key, amp_key, white_key = jax.random.split(base_key, 6)
    plane_sites = NY * NZ
    site_shape = (NT, NX, plane_sites)
    noise = jax.random.truncated_normal(noise_key, -4.0, 4.0, (2, 3, 3) + site_shape, jnp.float32)
    innovation = jax.random.truncated_normal(field_key, -4.0, 4.0, (NX, 2, plane_sites), jnp.float32)
    white = jax.random.truncated_normal(white_key, -4.0, 4.0, (2,) + site_shape, jnp.float32)
    strength = jax.random.uniform(scale_key, site_shape, jnp.float32, 4.0, 12.0)
    log_length = jax.random.uniform(rate_key, (plane_sites,), jnp.float32, 0.0, jnp.log(1.0 * NX))
    amplitude = jnp.exp(jax.random.uniform(amp_key, (plane_sites,), jnp.float32, jnp.log(0.4), jnp.log(1.2)))
    rate = jnp.exp(-jnp.exp(-log_length))
    field = along_planes(innovation, rate)
    phase_one = (amplitude * field[:, 0] / NT)[None] + 0.15 * white[0]
    phase_two = (amplitude * field[:, 1] / NT)[None] + 0.15 * white[1]
    phase_three = -(phase_one + phase_two)
    cos_rows = jnp.stack([jnp.cos(phase_one), jnp.cos(phase_two), jnp.cos(phase_three)])
    sin_rows = jnp.stack([jnp.sin(phase_one), jnp.sin(phase_two), jnp.sin(phase_three)])
    unit_matrix = jnp.eye(3, dtype=noise.dtype)[:, :, None, None, None]
    matrix_real = noise[0] + strength[None, None] * unit_matrix * cos_rows[:, None]
    matrix_imag = noise[1] + strength[None, None] * unit_matrix * sin_rows[:, None]
    first_real, first_imag = normalize(matrix_real[:, 0], matrix_imag[:, 0])
    second_real, second_imag = project(first_real, first_imag, matrix_real[:, 1], matrix_imag[:, 1])
    second_real, second_imag = normalize(second_real, second_imag)
    third_real, third_imag = project(first_real, first_imag, matrix_real[:, 2], matrix_imag[:, 2])
    third_real, third_imag = project(second_real, second_imag, third_real, third_imag)
    third_real, third_imag = normalize(third_real, third_imag)
    cross_real = []
    cross_imag = []
    for row_index in range(3):
        next_row = (row_index + 1) % 3
        last_row = (row_index + 2) % 3
        plus_real, plus_imag = times_complex(second_real[next_row], second_imag[next_row], third_real[last_row], third_imag[last_row])
        minus_real, minus_imag = times_complex(second_real[last_row], second_imag[last_row], third_real[next_row], third_imag[next_row])
        cross_real.append(plus_real - minus_real)
        cross_imag.append(plus_imag - minus_imag)
    det_real = jnp.zeros_like(cross_real[0])
    det_imag = jnp.zeros_like(cross_real[0])
    for row_index in range(3):
        term_real, term_imag = times_complex(first_real[row_index], first_imag[row_index], cross_real[row_index], cross_imag[row_index])
        det_real = det_real + term_real
        det_imag = det_imag + term_imag
    fixed_real, fixed_imag = times_complex(third_real, third_imag, det_real, -det_imag)
    whole_real = jnp.stack([first_real, second_real, fixed_real], axis=1)
    whole_imag = jnp.stack([first_imag, second_imag, fixed_imag], axis=1)
    matrix = jnp.stack([whole_real, whole_imag])
    return jnp.transpose(matrix, (3, 0, 1, 2, 4, 5))


def setup_inputs(seed: int = 0) -> dict:
    keys = jax.random.split(jax.random.key(seed), 2)
    return {
        "time_links": draw_time_links(jax.random.fold_in(keys[1], 71), 0),
    }


def complex_mul(left, right):
    terms_real = []
    terms_imag = []
    for middle in range(3):
        left_real = left[0][:, middle:middle + 1]
        left_imag = left[1][:, middle:middle + 1]
        right_real = right[0][middle:middle + 1]
        right_imag = right[1][middle:middle + 1]
        terms_real.append(left_real * right_real - left_imag * right_imag)
        terms_imag.append(left_real * right_imag + left_imag * right_real)
    return jnp.stack([terms_real[0] + terms_real[1] + terms_real[2], terms_imag[0] + terms_imag[1] + terms_imag[2]])


def trace_third(matrix):
    return (matrix[:, 0, 0] + matrix[:, 1, 1] + matrix[:, 2, 2]) / 3.0


def reference(time_links):
    product = time_links[0]
    for slice_index in range(1, NT):
        product = complex_mul(product, time_links[slice_index])
    loop_planes = jnp.transpose(trace_third(product), (1, 0, 2))
    columns = []
    for offset in range(RMAX + 1):
        rolled = jnp.roll(loop_planes, -offset, axis=0)
        columns.append(jnp.sum(loop_planes * rolled, axis=(1, 2)) / (NY * NZ))
    return loop_planes, jnp.stack(columns, axis=1)
```

```python
import functools

import jax
import jax.numpy as jnp
from jax import lax
from jax.experimental import pallas as pl
from jax.experimental.layout import Layout, with_layout_constraint
from jax.experimental.pallas import tpu as pltpu
from jax.sharding import Mesh, PartitionSpec as P

F32 = jnp.float32
LANES = 128
WIDE = pltpu.CompilerParams(vmem_limit_bytes=58 * 2**20)
SMALL = pltpu.CompilerParams(vmem_limit_bytes=12 * 2**20)


def cross_conj(first, second):
    row = []
    for k in range(3):
        a, b = (k + 1) % 3, (k + 2) % 3
        (fa, ga), (fb, gb) = first[a], first[b]
        (sa, ta), (sb, tb) = second[a], second[b]
        real = (fa * sb - ga * tb) - (fb * sa - gb * ta)
        imag = (fb * ta + gb * sa) - (fa * tb + ga * sb)
        row.append((real, imag))
    return row


def rows_times(rows, matrix):
    out = []
    for row in rows:
        line = []
        for j in range(3):
            real = imag = None
            for m in range(3):
                (ar, ai), (br, bi) = row[m], matrix[m][j]
                re = ar * br - ai * bi
                im = ar * bi + ai * br
                real = re if real is None else real + re
                imag = im if imag is None else imag + im
            line.append((real, imag))
        out.append(line)
    return out


CHUNKS = ((0, 8), (8, 8), (16, 2))


def product_kernel(links_ref, send_ref, keep_ref):
    mine = lax.axis_index("ta")
    for half, out_ref in ((1 - mine, send_ref), (mine, keep_ref)):
        for start, count in CHUNKS:
            def load(t, i, j):
                return tuple(
                    links_ref[t, i, j, pl.ds(36 * half + 2 * start + c, count, stride=2), :]
                    for c in range(2)
                )

            rows = [[load(0, i, j) for j in range(3)] for i in range(2)]
            for t in (1, 2):
                matrix = [[load(t, i, j) for j in range(3)] for i in range(2)]
                matrix.append(cross_conj(matrix[0], matrix[1]))
                rows = rows_times(rows, matrix)
            for i in range(2):
                for j in range(3):
                    for c in range(2):
                        out_ref[6 * i + 2 * j + c, 0, pl.ds(start, count), :] = rows[i][j][c]


def trace_kernel(keep_ref, got_ref, planes_ref, msg_ref):
    msg_ref[...] = jnp.zeros_like(msg_ref)
    for p in range(6):
        for start, count in CHUNKS:
            def load(ref):
                rows = [
                    [
                        tuple(ref[6 * i + 2 * j + c, p, pl.ds(start, count), :] for c in range(2))
                        for j in range(3)
                    ]
                    for i in range(2)
                ]
                rows.append(cross_conj(rows[0], rows[1]))
                return rows

            own, other = load(keep_ref), load(got_ref)
            real = imag = None
            for i in range(3):
                for j in range(3):
                    (ar, ai), (br, bi) = own[i][j], other[j][i]
                    re = ar * br - ai * bi
                    im = ar * bi + ai * br
                    real = re if real is None else real + re
                    imag = im if imag is None else imag + im
            base = 36 * p + 2 * start
            planes_ref[pl.ds(base, count, stride=2), :] = real / 3.0
            planes_ref[pl.ds(base + 1, count, stride=2), :] = imag / 3.0
    lane = lax.broadcasted_iota(jnp.int32, (4, LANES), 1) // 32
    tails = []
    for p in range(6):
        for c in range(2):
            for slot in range(2):
                count = 9 if c == 0 else 7
                tiles = planes_ref[pl.ds(36 * p + 2 * slot + c, count, stride=4), :]
                msg_ref[pl.ds(16 * 9 * c + 6 * slot + p, count, stride=16), :] = tiles
        tails.append(planes_ref[pl.ds(36 * p + 28 + 1, 4, stride=2), :])
    for b in range(4):
        for row, members in ((12, (0, 1, 2, 3)), (13, (4, 5))):
            packed = jnp.zeros((4, LANES), F32)
            for place, p in enumerate(members):
                shift = (32 * (place - b)) % LANES
                moved = pltpu.roll(tails[p], shift, 1) if shift else tails[p]
                packed = jnp.where(lane == place, moved, packed)
            msg_ref[pl.ds(16 * b + row, 4, stride=64), :] = packed


def correlate_kernel(own_ref, next_ref, far_ref, out_ref, rows_ref, shift_ref):
    lane = lax.broadcasted_iota(jnp.int32, (16, LANES), 1)
    for z, ref in enumerate((own_ref, next_ref, far_ref)):
        for p in range(6):
            target = pl.ds(96 * z + p, 16, stride=6)
            for k in range(2):
                rows_ref[k, target, :] = ref[pl.ds(6 * k + p, 16, stride=16), :]
            tail = ref[pl.ds(12 + p // 4, 16, stride=16), :]
            shift = (-32 * (p % 4)) % LANES
            tail = pltpu.roll(tail, shift, 1) if shift else tail
            rows_ref[2, target, :] = jnp.where(lane < 32, tail, 0.0)
    rows = jnp.concatenate([rows_ref[k] for k in range(3)], axis=1)
    products = lax.dot_general(
        rows[:96],
        rows,
        (((1,), (1,)), ((), ())),
        precision=lax.Precision.HIGHEST,
        preferred_element_type=F32,
    )
    products = jnp.concatenate([products, jnp.zeros((96, 96), F32)], axis=1)
    row = lax.broadcasted_iota(jnp.int32, (96, 384), 0)
    for bit in (1, 2, 4):
        products = jnp.where((row & bit) != 0, pltpu.roll(products, 384 - bit, 1), products)
    for g in range(12):
        group = products[8 * g : 8 * g + 8]
        if g:
            group = pltpu.roll(group, 384 - 8 * g, 1)
        for k in range(2):
            shift_ref[k, pl.ds(8 * g, 8), :] = group[:, LANES * k : LANES * (k + 1)]
    out_ref[...] = jnp.zeros_like(out_ref)
    for p in range(6):
        for k in range(2):
            out_ref[pl.ds(8 * k + p, 16, stride=16), :] = shift_ref[k, pl.ds(p, 16, stride=6), :]


def vmem(count):
    return [pl.BlockSpec(memory_space=pltpu.VMEM)] * count


def per_device(time_links):
    links = with_layout_constraint(
        time_links.reshape(3, 2, 3, 3, 6, 36, LANES),
        Layout((0, 2, 3, 4, 5, 1, 6)),
    )
    links = jnp.transpose(links, (0, 2, 3, 4, 5, 1, 6)).reshape(3, 3, 3, 432, LANES)
    send, keep = pl.pallas_call(
        product_kernel,
        grid=(6,),
        in_specs=[pl.BlockSpec((3, 2, 3, 72, LANES), lambda x: (0, 0, 0, x, 0))],
        out_specs=[pl.BlockSpec((12, 1, 18, LANES), lambda x: (0, x, 0, 0))] * 2,
        out_shape=[jax.ShapeDtypeStruct((12, 6, 18, LANES), F32)] * 2,
        compiler_params=WIDE,
        name="product",
    )(links)
    got = lax.ppermute(send, "ta", [(0, 1), (1, 0)])
    planes, messages = pl.pallas_call(
        trace_kernel,
        in_specs=vmem(2),
        out_specs=vmem(2),
        out_shape=[
            jax.ShapeDtypeStruct((216, LANES), F32),
            jax.ShapeDtypeStruct((256, LANES), F32),
        ],
        compiler_params=SMALL,
        name="trace",
    )(keep, got)
    loop_planes = with_layout_constraint(
        planes.reshape(6, 18, 2, LANES).transpose(0, 2, 1, 3),
        Layout((0, 2, 1, 3)),
    ).reshape(6, 2, 2304)
    own = lax.all_to_all(
        messages.reshape(16, 16, LANES), ("y", "x"), split_axis=0, concat_axis=0, tiled=True
    ).reshape(256, LANES)
    following = lax.ppermute(own, "z", [((d + 1) % 4, d) for d in range(4)])
    opposite = lax.ppermute(own, "z", [((d + 2) % 4, d) for d in range(4)])
    partial = pl.pallas_call(
        correlate_kernel,
        in_specs=vmem(3),
        out_specs=pl.BlockSpec(memory_space=pltpu.VMEM),
        out_shape=jax.ShapeDtypeStruct((256, LANES), F32),
        scratch_shapes=[pltpu.VMEM((3, 288, LANES), F32), pltpu.VMEM((2, 96, LANES), F32)],
        compiler_params=SMALL,
        name="correlate",
    )(own, following, opposite)
    pieces = lax.all_to_all(
        partial.reshape(16, 16, LANES), ("y", "x"), split_axis=0, concat_axis=0, tiled=True
    )
    total = jnp.sum(pieces, axis=0)
    total = total + lax.ppermute(total, "ta", [(0, 1), (1, 0)])
    correlator = jnp.concatenate([total[0:6], total[8:14, :65]], axis=1) / 4608.0
    return loop_planes, correlator


def solution(mesh):
    grid = Mesh(mesh.devices.reshape(2, 4, 4, 4), ("ta", "z", "y", "x"))
    gx = ("z", "y", "x")
    return jax.shard_map(
        per_device,
        mesh=grid,
        in_specs=(P("ta", None, None, None, gx, None),),
        out_specs=(P(gx, None, "ta"), P(gx, None)),
        check_vma=False,
    )
```

```python
import functools

import jax
import jax.numpy as jnp
from jax import lax
from jax.experimental import pallas as pl
from jax.experimental.layout import Layout, with_layout_constraint
from jax.experimental.pallas import tpu as pltpu
from jax.sharding import Mesh, PartitionSpec as P

F32 = jnp.float32
LANES = 128
WIDE = pltpu.CompilerParams(vmem_limit_bytes=50 * 2**20)
SMALL = pltpu.CompilerParams(vmem_limit_bytes=12 * 2**20)


def cross_conj(first, second):
    row = []
    for k in range(3):
        a, b = (k + 1) % 3, (k + 2) % 3
        (fa, ga), (fb, gb) = first[a], first[b]
        (sa, ta), (sb, tb) = second[a], second[b]
        real = (fa * sb - ga * tb) - (fb * sa - gb * ta)
        imag = (fb * ta + gb * sa) - (fa * tb + ga * sb)
        row.append((real, imag))
    return row


def rows_times(rows, matrix):
    out = []
    for row in rows:
        line = []
        for j in range(3):
            real = imag = None
            for m in range(3):
                (ar, ai), (br, bi) = row[m], matrix[m][j]
                re = ar * br - ai * bi
                im = ar * bi + ai * br
                real = re if real is None else real + re
                imag = im if imag is None else imag + im
            line.append((real, imag))
        out.append(line)
    return out


CHUNKS = ((0, 8), (8, 8), (16, 2))


def product_kernel(other, links_ref, out_ref, links, sems):
    half = lax.axis_index("ta")
    if other:
        half = 1 - half
    copies = []
    for x in range(6):
        source = pl.ds(pl.multiple_of(72 * x + 32 * half, 8), 40)
        copies.append(
            [
                pltpu.make_async_copy(
                    links_ref.at[t, pl.ds(0, 2), :, source, :], links.at[x, t], sems.at[x, t]
                )
                for t in range(3)
            ]
        )
        for copy in copies[x]:
            copy.start()
    for x in range(6):
        for copy in copies[x]:
            copy.wait()
        for start, count in CHUNKS:
            def load(t, i, j):
                return tuple(
                    links[x, t, i, j, pl.ds(4 * half + 2 * start + c, count, stride=2), :]
                    for c in range(2)
                )

            rows = [[load(0, i, j) for j in range(3)] for i in range(2)]
            for t in (1, 2):
                matrix = [[load(t, i, j) for j in range(3)] for i in range(2)]
                matrix.append(cross_conj(matrix[0], matrix[1]))
                rows = rows_times(rows, matrix)
            for i in range(2):
                for j in range(3):
                    for c in range(2):
                        out_ref[6 * i + 2 * j + c, x, pl.ds(start, count), :] = rows[i][j][c]


def product(links, other):
    return pl.pallas_call(
        functools.partial(product_kernel, other),
        in_specs=[pl.BlockSpec(memory_space=pltpu.HBM)],
        out_specs=pl.BlockSpec(memory_space=pltpu.VMEM),
        out_shape=jax.ShapeDtypeStruct((12, 6, 18, LANES), F32),
        scratch_shapes=[
            pltpu.VMEM((6, 3, 2, 3, 40, LANES), F32),
            pltpu.SemaphoreType.DMA((6, 3)),
        ],
        compiler_params=WIDE,
        cost_estimate=pl.CostEstimate(
            flops=40_000_000, bytes_accessed=2_000_000, transcendentals=0
        ),
        name="product_sent" if other else "product_kept",
    )(links)


def trace_kernel(keep_ref, got_ref, planes_ref, msg_ref):
    for d in range(16):
        msg_ref[0, pl.ds(16 * d + 8, 8), :] = jnp.zeros((8, LANES), F32)
    for p in range(6):
        for start, count in CHUNKS:
            def load(ref):
                rows = [
                    [
                        tuple(ref[6 * i + 2 * j + c, p, pl.ds(start, count), :] for c in range(2))
                        for j in range(3)
                    ]
                    for i in range(2)
                ]
                rows.append(cross_conj(rows[0], rows[1]))
                return rows

            own, other = load(keep_ref), load(got_ref)
            real = imag = None
            for i in range(3):
                for j in range(3):
                    (ar, ai), (br, bi) = own[i][j], other[j][i]
                    re = ar * br - ai * bi
                    im = ar * bi + ai * br
                    real = re if real is None else real + re
                    imag = im if imag is None else imag + im
            base = 36 * p + 2 * start
            planes_ref[pl.ds(base, count, stride=2), :] = real / 3.0
            planes_ref[pl.ds(base + 1, count, stride=2), :] = imag / 3.0
    lane = lax.broadcasted_iota(jnp.int32, (4, LANES), 1) // 32
    tails = []
    for p in range(6):
        for c in range(2):
            for slot in range(2):
                count = 9 if c == 0 else 7
                tiles = planes_ref[pl.ds(36 * p + 2 * slot + c, count, stride=4), :]
                msg_ref[0, pl.ds(16 * 9 * c + 6 * slot + p, count, stride=16), :] = tiles
        tails.append(planes_ref[pl.ds(36 * p + 28 + 1, 4, stride=2), :])
    for b in range(4):
        for row, members in ((12, (0, 1, 2, 3)), (13, (4, 5))):
            packed = jnp.zeros((4, LANES), F32)
            for place, p in enumerate(members):
                shift = (32 * (place - b)) % LANES
                moved = pltpu.roll(tails[p], shift, 1) if shift else tails[p]
                packed = jnp.where(lane == place, moved, packed)
            msg_ref[0, pl.ds(16 * b + row, 4, stride=64), :] = packed
    for z in range(1, 4):
        msg_ref[z] = msg_ref[0]


def correlate_kernel(got_ref, out_ref, rows_ref, shift_ref):
    mine = lax.axis_index("z")
    lane = lax.broadcasted_iota(jnp.int32, (16, LANES), 1)
    for z in range(3):
        block = (mine + z) % 4
        for p in range(6):
            target = pl.ds(96 * z + p, 16, stride=6)
            for k in range(2):
                rows_ref[k, target, :] = got_ref[block, pl.ds(6 * k + p, 16, stride=16), :]
            tail = got_ref[block, pl.ds(12 + p // 4, 16, stride=16), :]
            shift = (-32 * (p % 4)) % LANES
            tail = pltpu.roll(tail, shift, 1) if shift else tail
            rows_ref[2, target, :] = jnp.where(lane < 32, tail, 0.0)
    rows = jnp.concatenate([rows_ref[k] for k in range(3)], axis=1)
    products = lax.dot_general(
        rows[:96],
        rows,
        (((1,), (1,)), ((), ())),
        precision=lax.Precision.HIGHEST,
        preferred_element_type=F32,
    )
    products = jnp.concatenate([products, jnp.zeros((96, 96), F32)], axis=1)
    row = lax.broadcasted_iota(jnp.int32, (96, 384), 0)
    for bit in (1, 2, 4):
        products = jnp.where((row & bit) != 0, pltpu.roll(products, 384 - bit, 1), products)
    for g in range(12):
        group = products[8 * g : 8 * g + 8]
        if g:
            group = pltpu.roll(group, 384 - 8 * g, 1)
        for k in range(2):
            shift_ref[k, pl.ds(8 * g, 8), :] = group[:, LANES * k : LANES * (k + 1)]
    out_ref[...] = jnp.zeros_like(out_ref)
    for p in range(6):
        for k in range(2):
            out_ref[pl.ds(8 * k + p, 16, stride=16), :] = shift_ref[k, pl.ds(p, 16, stride=6), :]


def vmem(count):
    return [pl.BlockSpec(memory_space=pltpu.VMEM)] * count


def per_device(time_links):
    links = with_layout_constraint(
        time_links.reshape(3, 2, 3, 3, 6, 36, LANES),
        Layout((0, 2, 3, 4, 5, 1, 6)),
    )
    links = jnp.transpose(links, (0, 2, 3, 4, 5, 1, 6)).reshape(3, 3, 3, 432, LANES)
    got = lax.ppermute(product(links, True), "ta", [(0, 1), (1, 0)])
    keep = product(links, False)
    planes, messages = pl.pallas_call(
        trace_kernel,
        in_specs=vmem(2),
        out_specs=vmem(2),
        out_shape=[
            jax.ShapeDtypeStruct((216, LANES), F32),
            jax.ShapeDtypeStruct((4, 256, LANES), F32),
        ],
        compiler_params=SMALL,
        name="trace",
    )(keep, got)
    loop_planes = with_layout_constraint(
        planes.reshape(6, 18, 2, LANES).transpose(0, 2, 1, 3),
        Layout((0, 2, 1, 3)),
    ).reshape(6, 2, 2304)
    gathered = lax.all_to_all(
        messages.reshape(64, 16, LANES), ("z", "y", "x"), split_axis=0, concat_axis=0, tiled=True
    ).reshape(4, 256, LANES)
    partial = pl.pallas_call(
        correlate_kernel,
        in_specs=vmem(1),
        out_specs=pl.BlockSpec(memory_space=pltpu.VMEM),
        out_shape=jax.ShapeDtypeStruct((256, LANES), F32),
        scratch_shapes=[pltpu.VMEM((3, 288, LANES), F32), pltpu.VMEM((2, 96, LANES), F32)],
        compiler_params=SMALL,
        name="correlate",
    )(gathered)
    pieces = lax.all_to_all(
        partial.reshape(16, 16, LANES), ("y", "x"), split_axis=0, concat_axis=0, tiled=True
    )
    total = jnp.sum(pieces, axis=0)
    total = total + lax.ppermute(total, "ta", [(0, 1), (1, 0)])
    correlator = jnp.concatenate([total[0:6], total[8:14, :65]], axis=1) / 4608.0
    return loop_planes, correlator


def solution(mesh):
    grid = Mesh(mesh.devices.reshape(2, 4, 4, 4), ("ta", "z", "y", "x"))
    gx = ("z", "y", "x")
    return jax.shard_map(
        per_device,
        mesh=grid,
        in_specs=(P("ta", None, None, None, gx, None),),
        out_specs=(P(gx, None, "ta"), P(gx, None)),
        check_vma=False,
    )
```

```python
import functools

import jax
import jax.numpy as jnp
from jax import lax
from jax.experimental import pallas as pl
from jax.experimental.layout import Layout, with_layout_constraint
from jax.experimental.pallas import tpu as pltpu
from jax.sharding import Mesh, PartitionSpec as P

F32 = jnp.float32
LANES = 128
WIDE = pltpu.CompilerParams(vmem_limit_bytes=50 * 2**20)
SMALL = pltpu.CompilerParams(vmem_limit_bytes=12 * 2**20)


def cross_conj(first, second):
    row = []
    for k in range(3):
        a, b = (k + 1) % 3, (k + 2) % 3
        (fa, ga), (fb, gb) = first[a], first[b]
        (sa, ta), (sb, tb) = second[a], second[b]
        real = (fa * sb - ga * tb) - (fb * sa - gb * ta)
        imag = (fb * ta + gb * sa) - (fa * tb + ga * sb)
        row.append((real, imag))
    return row


def rows_times(rows, matrix):
    out = []
    for row in rows:
        line = []
        for j in range(3):
            real = imag = None
            for m in range(3):
                (ar, ai), (br, bi) = row[m], matrix[m][j]
                re = ar * br - ai * bi
                im = ar * bi + ai * br
                real = re if real is None else real + re
                imag = im if imag is None else imag + im
            line.append((real, imag))
        out.append(line)
    return out


THIRD = 1.0 / 3.0
MSG = 14
RES = 10
CHUNKS = ((0, 8), (8, 8), (16, 2))


def half_reads(half, links_ref, links, sems):
    copies = []
    for x in range(6):
        source = pl.ds(pl.multiple_of(72 * x + 32 * half, 8), 40)
        copies.append(
            pltpu.make_async_copy(
                links_ref.at[:, pl.ds(0, 2), :, source, :], links.at[x], sems.at[x, 0]
            )
        )
    return copies


def multiply_half(half, links, out_ref, x):
    for start, count in CHUNKS:
        def load(t, i, j):
            return tuple(
                links[x, t, i, j, pl.ds(4 * half + 2 * start + c, count, stride=2), :]
                for c in range(2)
            )

        rows = [[load(0, i, j) for j in range(3)] for i in range(2)]
        for t in (1, 2):
            matrix = [[load(t, i, j) for j in range(3)] for i in range(2)]
            matrix.append(cross_conj(matrix[0], matrix[1]))
            rows = rows_times(rows, matrix)
        if out_ref.shape[0] == 18:
            rows.append(cross_conj(rows[0], rows[1]))
            rows = [[(re * THIRD, im * THIRD) for re, im in row] for row in rows]
        for i, row in enumerate(rows):
            for j in range(3):
                for c in range(2):
                    out_ref[6 * i + 2 * j + c, pl.ds(18 * x + start, count), :] = row[j][c]


def product_kernel(other, links_ref, out_ref, links, sems):
    half = lax.axis_index("ta")
    half = 1 - half if other else half
    copies = half_reads(half, links_ref, links, sems)
    for copy in copies:
        copy.start()
    for x in range(6):
        for copy in copies[x : x + 1]:
            copy.wait()
        multiply_half(half, links, out_ref, x)


def product(links, other):
    return pl.pallas_call(
        functools.partial(product_kernel, other),
        in_specs=[pl.BlockSpec(memory_space=pltpu.HBM)],
        out_specs=pl.BlockSpec(memory_space=pltpu.VMEM),
        out_shape=jax.ShapeDtypeStruct((12 if other else 18, 108, LANES), F32),
        scratch_shapes=[
            pltpu.VMEM((6, 3, 2, 3, 40, LANES), F32),
            pltpu.SemaphoreType.DMA((6, 3)),
        ],
        compiler_params=WIDE,
        cost_estimate=pl.CostEstimate(
            flops=40_000_000, bytes_accessed=2_000_000, transcendentals=0
        ),
        name="product_sent" if other else "product_kept",
    )(links)


def trace_kernel(keep_ref, got_ref, planes_ref, msg_ref):
    for start in range(0, 108, 8):
        count = min(8, 108 - start)

        def load(ref, rows):
            return [
                [
                    tuple(ref[6 * i + 2 * j + c, pl.ds(start, count), :] for c in range(2))
                    for j in range(3)
                ]
                for i in range(rows)
            ]

        own, other = load(keep_ref, 3), load(got_ref, 2)
        other.append(cross_conj(other[0], other[1]))
        real = imag = None
        for i in range(3):
            for j in range(3):
                (ar, ai), (br, bi) = own[i][j], other[j][i]
                re = ar * br - ai * bi
                im = ar * bi + ai * br
                real = re if real is None else real + re
                imag = im if imag is None else imag + im
        planes_ref[pl.ds(2 * start, count, stride=2), :] = real
        planes_ref[pl.ds(2 * start + 1, count, stride=2), :] = imag
    lane = lax.broadcasted_iota(jnp.int32, (4, LANES), 1) // 32
    tails = []
    for p in range(6):
        for c in range(2):
            for slot in range(2):
                count = 9 if c == 0 else 7
                tiles = planes_ref[pl.ds(36 * p + 2 * slot + c, count, stride=4), :]
                msg_ref[0, pl.ds(MSG * 9 * c + 6 * slot + p, count, stride=MSG), :] = tiles
        tails.append(planes_ref[pl.ds(36 * p + 28 + 1, 4, stride=2), :])
    for b in range(4):
        for row, members in ((12, (0, 1, 2, 3)), (13, (4, 5))):
            packed = jnp.zeros((4, LANES), F32)
            for place, p in enumerate(members):
                shift = (32 * (place - b)) % LANES
                moved = pltpu.roll(tails[p], shift, 1) if shift else tails[p]
                packed = jnp.where(lane == place, moved, packed)
            msg_ref[0, pl.ds(MSG * b + row, 4, stride=4 * MSG), :] = packed
    for z in range(1, 4):
        msg_ref[z] = msg_ref[0]


def dot_rows(left, right):
    return lax.dot_general(
        left, right, (((1,), (1,)), ((), ())), preferred_element_type=F32
    )


def correlate_kernel(got_ref, planes_ref, out_ref, result_ref, rows_ref, shift_ref, sem):
    write = pltpu.make_async_copy(planes_ref, result_ref, sem)
    write.start()
    mine = lax.axis_index("z")

    @pl.when(mine < 4)
    def _():
        correlate(mine, got_ref, out_ref, rows_ref, shift_ref)

    write.wait()


def correlate(mine, got_ref, out_ref, rows_ref, shift_ref):
    lane = lax.broadcasted_iota(jnp.int32, (16, LANES), 1)
    for z in range(3):
        block = (mine + z) % 4
        for p in range(6):
            target = pl.ds(96 * z + p, 16, stride=6)
            for k in range(2):
                rows_ref[k, target, :] = got_ref[block, pl.ds(6 * k + p, 16, stride=MSG), :]
            tail = got_ref[block, pl.ds(12 + p // 4, 16, stride=MSG), :]
            shift = (-32 * (p % 4)) % LANES
            tail = pltpu.roll(tail, shift, 1) if shift else tail
            rows_ref[2, target, :] = jnp.where(lane < 32, tail, 0.0)
    rows = jnp.concatenate([rows_ref[k] for k in range(3)], axis=1)
    high = rows.astype(jnp.bfloat16)
    low = (rows - high.astype(F32)).astype(jnp.bfloat16)
    both = dot_rows(jnp.concatenate([high[:96], low[:96]], axis=0), high)
    products = both[:96] + (both[96:] + dot_rows(high[:96], low))
    products = jnp.concatenate([products, jnp.zeros((96, 96), F32)], axis=1)
    row = lax.broadcasted_iota(jnp.int32, (96, 384), 0)
    for bit in (1, 2, 4):
        products = jnp.where((row & bit) != 0, pltpu.roll(products, 384 - bit, 1), products)
    for g in range(12):
        group = products[8 * g : 8 * g + 8]
        if g:
            group = pltpu.roll(group, 384 - 8 * g, 1)
        for k in range(2):
            shift_ref[k, pl.ds(8 * g, 8), :] = group[:, LANES * k : LANES * (k + 1)]
    far = []
    for p in range(6):
        out_ref[0, pl.ds(p, 16, stride=RES), :] = shift_ref[0, pl.ds(p, 16, stride=6), :]
        far.append(shift_ref[1, pl.ds(p, 16, stride=6), :])
    last = jnp.zeros((16, LANES), F32)
    for p in range(6):
        last = jnp.where(lane == p, pltpu.roll(far[p], 64 + p, 1), last)
    out_ref[0, pl.ds(9, 16, stride=RES), :] = last
    for q in range(3):
        pair = jnp.where(lane < 64, far[2 * q], pltpu.roll(far[2 * q + 1], 64, 1))
        out_ref[0, pl.ds(6 + q, 16, stride=RES), :] = pair
    out_ref[1] = out_ref[0]


def total_kernel(pieces_ref, out_ref):
    sums = [
        jnp.sum(pieces_ref[pl.ds(k, 32, stride=RES), :], axis=0, keepdims=True) * (1.0 / 4608.0)
        for k in range(RES)
    ]
    lane = lax.broadcasted_iota(jnp.int32, (1, LANES), 1)
    for p in range(6):
        out_ref[pl.ds(p, 1), pl.ds(0, LANES)] = sums[p]
        far = sums[6 + p // 2]
        far = pltpu.roll(far, 64, 1) if p % 2 else far
        far = jnp.where(lane < 64, far, pltpu.roll(sums[9], 64 - p, 1))
        out_ref[pl.ds(p, 1), pl.ds(LANES, 65)] = far[:, :65]


def vmem(count):
    return [pl.BlockSpec(memory_space=pltpu.VMEM)] * count


def per_device(time_links):
    links = with_layout_constraint(
        time_links.reshape(3, 2, 3, 3, 6, 36, LANES),
        Layout((0, 2, 3, 4, 5, 1, 6)),
    )
    links = jnp.transpose(links, (0, 2, 3, 4, 5, 1, 6)).reshape(3, 3, 3, 432, LANES)
    got = lax.ppermute(product(links, True), "ta", [(0, 1), (1, 0)])
    keep = product(links, False)
    planes, messages = pl.pallas_call(
        trace_kernel,
        in_specs=vmem(2),
        out_specs=vmem(2),
        out_shape=[
            jax.ShapeDtypeStruct((216, LANES), F32),
            jax.ShapeDtypeStruct((4, 16 * MSG, LANES), F32),
        ],
        compiler_params=SMALL,
        name="trace",
    )(keep, got)
    gathered = exchange(messages, ("z", "y", "x"), MSG)
    partial, planes = pl.pallas_call(
        correlate_kernel,
        in_specs=vmem(2),
        out_specs=vmem(1) + [pl.BlockSpec(memory_space=pltpu.HBM)],
        out_shape=[
            jax.ShapeDtypeStruct((2, 16 * RES, LANES), F32),
            jax.ShapeDtypeStruct((216, LANES), F32),
        ],
        scratch_shapes=[
            pltpu.VMEM((3, 288, LANES), F32),
            pltpu.VMEM((2, 96, LANES), F32),
            pltpu.SemaphoreType.DMA,
        ],
        compiler_params=SMALL,
        name="correlate",
    )(gathered, planes)
    loop_planes = with_layout_constraint(
        planes.reshape(6, 18, 2, LANES).transpose(0, 2, 1, 3),
        Layout((0, 2, 1, 3)),
    ).reshape(6, 2, 2304)
    pieces = exchange(partial, ("ta", "y", "x"), RES)
    correlator = pl.pallas_call(
        total_kernel,
        in_specs=vmem(1),
        out_specs=pl.BlockSpec(memory_space=pltpu.VMEM),
        out_shape=jax.ShapeDtypeStruct((6, 193), F32),
        compiler_params=SMALL,
        name="total",
    )(pieces.reshape(32 * RES, LANES))
    return loop_planes, correlator


def exchange(values, axes, rows):
    shape = values.shape
    values = values.reshape(-1, rows // 2, 2, LANES)
    return lax.all_to_all(values, axes, split_axis=0, concat_axis=0, tiled=True).reshape(shape)


def solution(mesh):
    grid = Mesh(mesh.devices.reshape(2, 4, 4, 4), ("ta", "z", "y", "x"))
    gx = ("z", "y", "x")
    return jax.shard_map(
        per_device,
        mesh=grid,
        in_specs=(P("ta", None, None, None, gx, None),),
        out_specs=(P(gx, None, "ta"), P(gx, None)),
        check_vma=False,
    )
```

```python
import functools

import jax
import jax.numpy as jnp
from jax import lax
from jax.experimental import pallas as pl
from jax.experimental.layout import Layout, with_layout_constraint
from jax.experimental.pallas import tpu as pltpu
from jax.sharding import Mesh, PartitionSpec as P

F32 = jnp.float32
LANES = 128
WIDE = pltpu.CompilerParams(vmem_limit_bytes=50 * 2**20)
SMALL = pltpu.CompilerParams(vmem_limit_bytes=12 * 2**20)


def cross_conj(first, second):
    row = []
    for k in range(3):
        a, b = (k + 1) % 3, (k + 2) % 3
        (fa, ga), (fb, gb) = first[a], first[b]
        (sa, ta), (sb, tb) = second[a], second[b]
        real = (fa * sb - ga * tb) - (fb * sa - gb * ta)
        imag = (fb * ta + gb * sa) - (fa * tb + ga * sb)
        row.append((real, imag))
    return row


def rows_times(rows, matrix):
    out = []
    for row in rows:
        line = []
        for j in range(3):
            real = imag = None
            for m in range(3):
                (ar, ai), (br, bi) = row[m], matrix[m][j]
                re = ar * br - ai * bi
                im = ar * bi + ai * br
                real = re if real is None else real + re
                imag = im if imag is None else imag + im
            line.append((real, imag))
        out.append(line)
    return out


THIRD = 1.0 / 3.0
MSG = 14
RES = 10
CHUNKS = ((0, 8), (8, 8), (16, 2))


def half_reads(half, links_ref, links, sems, planes=range(6)):
    copies = []
    for i, x in enumerate(planes):
        source = pl.ds(pl.multiple_of(72 * x + 32 * half, 8), 40)
        copies.append(
            pltpu.make_async_copy(
                links_ref.at[:, pl.ds(0, 2), :, source, :], links.at[i], sems.at[i]
            )
        )
    return copies


def multiply_half(half, links, out_ref, x, place):
    for start, count in CHUNKS:
        def load(t, i, j):
            return tuple(
                links[place, t, i, j, pl.ds(4 * half + 2 * start + c, count, stride=2), :]
                for c in range(2)
            )

        rows = [[load(0, i, j) for j in range(3)] for i in range(2)]
        for t in (1, 2):
            matrix = [[load(t, i, j) for j in range(3)] for i in range(2)]
            matrix.append(cross_conj(matrix[0], matrix[1]))
            rows = rows_times(rows, matrix)
        if out_ref.shape[0] == 18:
            rows.append(cross_conj(rows[0], rows[1]))
            rows = [[(re * THIRD, im * THIRD) for re, im in row] for row in rows]
        for i, row in enumerate(rows):
            for j in range(3):
                for c in range(2):
                    out_ref[6 * i + 2 * j + c, pl.ds(18 * x + start, count), :] = row[j][c]


EARLY = 2


def sent_kernel(links_ref, out_ref, early, links, sems, early_sems):
    mine = lax.axis_index("ta")
    copies = half_reads(1 - mine, links_ref, links, sems)
    ahead = half_reads(mine, links_ref, early, early_sems, range(EARLY))
    for copy in copies + ahead:
        copy.start()
    for x in range(6):
        copies[x].wait()
        multiply_half(1 - mine, links, out_ref, x, x)
    for copy in ahead:
        copy.wait()


def kept_kernel(links_ref, early, out_ref, links, sems):
    mine = lax.axis_index("ta")
    copies = half_reads(mine, links_ref, links, sems, range(EARLY, 6))
    for copy in copies:
        copy.start()
    for x in range(EARLY):
        multiply_half(mine, early, out_ref, x, x)
    for x in range(EARLY, 6):
        copies[x - EARLY].wait()
        multiply_half(mine, links, out_ref, x, x - EARLY)


def product(links):
    hbm = [pl.BlockSpec(memory_space=pltpu.HBM)]
    cost = pl.CostEstimate(flops=40_000_000, bytes_accessed=2_000_000, transcendentals=0)
    sent, early = pl.pallas_call(
        sent_kernel,
        in_specs=hbm,
        out_specs=vmem(2),
        out_shape=[
            jax.ShapeDtypeStruct((12, 108, LANES), F32),
            jax.ShapeDtypeStruct((EARLY, 3, 2, 3, 40, LANES), F32),
        ],
        scratch_shapes=[
            pltpu.VMEM((6, 3, 2, 3, 40, LANES), F32),
            pltpu.SemaphoreType.DMA((6,)),
            pltpu.SemaphoreType.DMA((EARLY,)),
        ],
        compiler_params=WIDE,
        cost_estimate=cost,
        name="product_sent",
    )(links)
    got = lax.ppermute(sent, "ta", [(0, 1), (1, 0)])
    keep = pl.pallas_call(
        kept_kernel,
        in_specs=hbm + vmem(1),
        out_specs=pl.BlockSpec(memory_space=pltpu.VMEM),
        out_shape=jax.ShapeDtypeStruct((18, 108, LANES), F32),
        scratch_shapes=[
            pltpu.VMEM((6 - EARLY, 3, 2, 3, 40, LANES), F32),
            pltpu.SemaphoreType.DMA((6 - EARLY,)),
        ],
        compiler_params=WIDE,
        cost_estimate=cost,
        name="product_kept",
    )(links, early)
    return keep, got


def trace_kernel(keep_ref, got_ref, planes_ref, msg_ref):
    for start in range(0, 108, 8):
        count = min(8, 108 - start)

        def load(ref, rows):
            return [
                [
                    tuple(ref[6 * i + 2 * j + c, pl.ds(start, count), :] for c in range(2))
                    for j in range(3)
                ]
                for i in range(rows)
            ]

        own, other = load(keep_ref, 3), load(got_ref, 2)
        other.append(cross_conj(other[0], other[1]))
        real = imag = None
        for i in range(3):
            for j in range(3):
                (ar, ai), (br, bi) = own[i][j], other[j][i]
                re = ar * br - ai * bi
                im = ar * bi + ai * br
                real = re if real is None else real + re
                imag = im if imag is None else imag + im
        planes_ref[pl.ds(2 * start, count, stride=2), :] = real
        planes_ref[pl.ds(2 * start + 1, count, stride=2), :] = imag
    lane = lax.broadcasted_iota(jnp.int32, (4, LANES), 1) // 32
    tails = []
    for p in range(6):
        for c in range(2):
            for slot in range(2):
                count = 9 if c == 0 else 7
                tiles = planes_ref[pl.ds(36 * p + 2 * slot + c, count, stride=4), :]
                msg_ref[0, pl.ds(MSG * 9 * c + 6 * slot + p, count, stride=MSG), :] = tiles
        tails.append(planes_ref[pl.ds(36 * p + 28 + 1, 4, stride=2), :])
    for b in range(4):
        for row, members in ((12, (0, 1, 2, 3)), (13, (4, 5))):
            packed = jnp.zeros((4, LANES), F32)
            for place, p in enumerate(members):
                shift = (32 * (place - b)) % LANES
                moved = pltpu.roll(tails[p], shift, 1) if shift else tails[p]
                packed = jnp.where(lane == place, moved, packed)
            msg_ref[0, pl.ds(MSG * b + row, 4, stride=4 * MSG), :] = packed
    for z in range(1, 4):
        msg_ref[z] = msg_ref[0]


def dot_rows(left, right):
    return lax.dot_general(
        left, right, (((1,), (1,)), ((), ())), preferred_element_type=F32
    )


def correlate_kernel(got_ref, planes_ref, out_ref, result_ref, rows_ref, shift_ref, sem):
    write = pltpu.make_async_copy(planes_ref, result_ref, sem)
    write.start()
    mine = lax.axis_index("z")

    @pl.when(mine < 4)
    def _():
        correlate(mine, got_ref, out_ref, rows_ref, shift_ref)

    write.wait()


def correlate(mine, got_ref, out_ref, rows_ref, shift_ref):
    lane = lax.broadcasted_iota(jnp.int32, (16, LANES), 1)
    for z in range(3):
        block = (mine + z) % 4
        for p in range(6):
            target = pl.ds(96 * z + p, 16, stride=6)
            for k in range(2):
                rows_ref[k, target, :] = got_ref[block, pl.ds(6 * k + p, 16, stride=MSG), :]
            tail = got_ref[block, pl.ds(12 + p // 4, 16, stride=MSG), :]
            shift = (-32 * (p % 4)) % LANES
            tail = pltpu.roll(tail, shift, 1) if shift else tail
            rows_ref[2, target, :] = jnp.where(lane < 32, tail, 0.0)
    rows = jnp.concatenate([rows_ref[k] for k in range(3)], axis=1)
    high = rows.astype(jnp.bfloat16)
    low = (rows - high.astype(F32)).astype(jnp.bfloat16)
    both = dot_rows(jnp.concatenate([high[:96], low[:96]], axis=0), high)
    products = both[:96] + (both[96:] + dot_rows(high[:96], low))
    products = jnp.concatenate([products, jnp.zeros((96, 96), F32)], axis=1)
    row = lax.broadcasted_iota(jnp.int32, (96, 384), 0)
    for bit in (1, 2, 4):
        products = jnp.where((row & bit) != 0, pltpu.roll(products, 384 - bit, 1), products)
    for g in range(12):
        group = products[8 * g : 8 * g + 8]
        if g:
            group = pltpu.roll(group, 384 - 8 * g, 1)
        for k in range(2):
            shift_ref[k, pl.ds(8 * g, 8), :] = group[:, LANES * k : LANES * (k + 1)]
    far = []
    for p in range(6):
        out_ref[0, pl.ds(p, 16, stride=RES), :] = shift_ref[0, pl.ds(p, 16, stride=6), :]
        far.append(shift_ref[1, pl.ds(p, 16, stride=6), :])
    last = jnp.zeros((16, LANES), F32)
    for p in range(6):
        last = jnp.where(lane == p, pltpu.roll(far[p], 64 + p, 1), last)
    out_ref[0, pl.ds(9, 16, stride=RES), :] = last
    for q in range(3):
        pair = jnp.where(lane < 64, far[2 * q], pltpu.roll(far[2 * q + 1], 64, 1))
        out_ref[0, pl.ds(6 + q, 16, stride=RES), :] = pair
    out_ref[1] = out_ref[0]


def total_kernel(pieces_ref, out_ref):
    sums = [
        jnp.sum(pieces_ref[pl.ds(k, 32, stride=RES), :], axis=0, keepdims=True) * (1.0 / 4608.0)
        for k in range(RES)
    ]
    lane = lax.broadcasted_iota(jnp.int32, (1, LANES), 1)
    for p in range(6):
        out_ref[pl.ds(p, 1), pl.ds(0, LANES)] = sums[p]
        far = sums[6 + p // 2]
        far = pltpu.roll(far, 64, 1) if p % 2 else far
        far = jnp.where(lane < 64, far, pltpu.roll(sums[9], 64 - p, 1))
        out_ref[pl.ds(p, 1), pl.ds(LANES, 65)] = far[:, :65]


def vmem(count):
    return [pl.BlockSpec(memory_space=pltpu.VMEM)] * count


def per_device(time_links):
    links = with_layout_constraint(
        time_links.reshape(3, 2, 3, 3, 6, 36, LANES),
        Layout((0, 2, 3, 4, 5, 1, 6)),
    )
    links = jnp.transpose(links, (0, 2, 3, 4, 5, 1, 6)).reshape(3, 3, 3, 432, LANES)
    keep, got = product(links)
    planes, messages = pl.pallas_call(
        trace_kernel,
        in_specs=vmem(2),
        out_specs=vmem(2),
        out_shape=[
            jax.ShapeDtypeStruct((216, LANES), F32),
            jax.ShapeDtypeStruct((4, 16 * MSG, LANES), F32),
        ],
        compiler_params=SMALL,
        name="trace",
    )(keep, got)
    gathered = exchange(messages, ("z", "y", "x"), MSG)
    partial, planes = pl.pallas_call(
        correlate_kernel,
        in_specs=vmem(2),
        out_specs=vmem(1) + [pl.BlockSpec(memory_space=pltpu.HBM)],
        out_shape=[
            jax.ShapeDtypeStruct((2, 16 * RES, LANES), F32),
            jax.ShapeDtypeStruct((216, LANES), F32),
        ],
        scratch_shapes=[
            pltpu.VMEM((3, 288, LANES), F32),
            pltpu.VMEM((2, 96, LANES), F32),
            pltpu.SemaphoreType.DMA,
        ],
        compiler_params=SMALL,
        name="correlate",
    )(gathered, planes)
    loop_planes = with_layout_constraint(
        planes.reshape(6, 18, 2, LANES).transpose(0, 2, 1, 3),
        Layout((0, 2, 1, 3)),
    ).reshape(6, 2, 2304)
    pieces = exchange(partial, ("ta", "y", "x"), RES)
    correlator = pl.pallas_call(
        total_kernel,
        in_specs=vmem(1),
        out_specs=pl.BlockSpec(memory_space=pltpu.VMEM),
        out_shape=jax.ShapeDtypeStruct((6, 193), F32),
        compiler_params=SMALL,
        name="total",
    )(pieces.reshape(32 * RES, LANES))
    return loop_planes, correlator


def exchange(values, axes, rows):
    shape = values.shape
    values = values.reshape(-1, rows // 2, 2, LANES)
    return lax.all_to_all(values, axes, split_axis=0, concat_axis=0, tiled=True).reshape(shape)


def solution(mesh):
    grid = Mesh(mesh.devices.reshape(2, 4, 4, 4), ("ta", "z", "y", "x"))
    gx = ("z", "y", "x")
    return jax.shard_map(
        per_device,
        mesh=grid,
        in_specs=(P("ta", None, None, None, gx, None),),
        out_specs=(P(gx, None, "ta"), P(gx, None)),
        check_vma=False,
    )
```

```python
import functools

import jax
import jax.numpy as jnp
from jax import lax
from jax.experimental import pallas as pl
from jax.experimental.layout import Layout, with_layout_constraint
from jax.experimental.pallas import tpu as pltpu
from jax.sharding import Mesh, PartitionSpec as P

F32 = jnp.float32
LANES = 128
WIDE = pltpu.CompilerParams(vmem_limit_bytes=50 * 2**20)
SMALL = pltpu.CompilerParams(vmem_limit_bytes=12 * 2**20)


def cross_conj(first, second):
    row = []
    for k in range(3):
        a, b = (k + 1) % 3, (k + 2) % 3
        (fa, ga), (fb, gb) = first[a], first[b]
        (sa, ta), (sb, tb) = second[a], second[b]
        real = (fa * sb - ga * tb) - (fb * sa - gb * ta)
        imag = (fb * ta + gb * sa) - (fa * tb + ga * sb)
        row.append((real, imag))
    return row


def rows_times(rows, matrix):
    out = []
    for row in rows:
        line = []
        for j in range(3):
            real = imag = None
            for m in range(3):
                (ar, ai), (br, bi) = row[m], matrix[m][j]
                re = ar * br - ai * bi
                im = ar * bi + ai * br
                real = re if real is None else real + re
                imag = im if imag is None else imag + im
            line.append((real, imag))
        out.append(line)
    return out


THIRD = 1.0 / 3.0
MSG = 7
RES = 10
CHUNKS = ((0, 8), (8, 8), (16, 2))


def half_reads(half, links_ref, links, sems, planes=range(6)):
    copies = []
    for i, x in enumerate(planes):
        source = pl.ds(pl.multiple_of(72 * x + 32 * half, 8), 40)
        copies.append(
            pltpu.make_async_copy(
                links_ref.at[:, pl.ds(0, 2), :, source, :], links.at[i], sems.at[i]
            )
        )
    return copies


def multiply_half(half, links, out_ref, x, place):
    for start, count in CHUNKS:
        def load(t, i, j):
            return tuple(
                links[place, t, i, j, pl.ds(4 * half + 2 * start + c, count, stride=2), :]
                for c in range(2)
            )

        rows = [[load(0, i, j) for j in range(3)] for i in range(2)]
        for t in (1, 2):
            matrix = [[load(t, i, j) for j in range(3)] for i in range(2)]
            matrix.append(cross_conj(matrix[0], matrix[1]))
            rows = rows_times(rows, matrix)
        if out_ref.shape[0] == 18:
            rows.append(cross_conj(rows[0], rows[1]))
            rows = [[(re * THIRD, im * THIRD) for re, im in row] for row in rows]
        for i, row in enumerate(rows):
            for j in range(3):
                for c in range(2):
                    out_ref[6 * i + 2 * j + c, pl.ds(18 * x + start, count), :] = row[j][c]


EARLY = 2


def sent_kernel(links_ref, out_ref, early, links, sems, early_sems):
    mine = lax.axis_index("ta")
    copies = half_reads(1 - mine, links_ref, links, sems)
    ahead = half_reads(mine, links_ref, early, early_sems, range(EARLY))
    for copy in copies + ahead:
        copy.start()
    for x in range(6):
        copies[x].wait()
        multiply_half(1 - mine, links, out_ref, x, x)
    for copy in ahead:
        copy.wait()


def kept_kernel(links_ref, early, out_ref, links, sems):
    mine = lax.axis_index("ta")
    copies = half_reads(mine, links_ref, links, sems, range(EARLY, 6))
    for copy in copies:
        copy.start()
    for x in range(EARLY):
        multiply_half(mine, early, out_ref, x, x)
    for x in range(EARLY, 6):
        copies[x - EARLY].wait()
        multiply_half(mine, links, out_ref, x, x - EARLY)


def product(links):
    hbm = [pl.BlockSpec(memory_space=pltpu.HBM)]
    cost = pl.CostEstimate(flops=40_000_000, bytes_accessed=2_000_000, transcendentals=0)
    sent, early = pl.pallas_call(
        sent_kernel,
        in_specs=hbm,
        out_specs=vmem(2),
        out_shape=[
            jax.ShapeDtypeStruct((12, 108, LANES), F32),
            jax.ShapeDtypeStruct((EARLY, 3, 2, 3, 40, LANES), F32),
        ],
        scratch_shapes=[
            pltpu.VMEM((6, 3, 2, 3, 40, LANES), F32),
            pltpu.SemaphoreType.DMA((6,)),
            pltpu.SemaphoreType.DMA((EARLY,)),
        ],
        compiler_params=WIDE,
        cost_estimate=cost,
        name="product_sent",
    )(links)
    got = lax.ppermute(sent, "ta", [(0, 1), (1, 0)])
    keep = pl.pallas_call(
        kept_kernel,
        in_specs=hbm + vmem(1),
        out_specs=pl.BlockSpec(memory_space=pltpu.VMEM),
        out_shape=jax.ShapeDtypeStruct((18, 108, LANES), F32),
        scratch_shapes=[
            pltpu.VMEM((6 - EARLY, 3, 2, 3, 40, LANES), F32),
            pltpu.SemaphoreType.DMA((6 - EARLY,)),
        ],
        compiler_params=WIDE,
        cost_estimate=cost,
        name="product_kept",
    )(links, early)
    return keep, got


def trace_kernel(keep_ref, got_ref, planes_ref, msg_ref):
    for start in range(0, 108, 8):
        count = min(8, 108 - start)

        def load(ref, rows):
            return [
                [
                    tuple(ref[6 * i + 2 * j + c, pl.ds(start, count), :] for c in range(2))
                    for j in range(3)
                ]
                for i in range(rows)
            ]

        own, other = load(keep_ref, 3), load(got_ref, 2)
        other.append(cross_conj(other[0], other[1]))
        real = imag = None
        for i in range(3):
            for j in range(3):
                (ar, ai), (br, bi) = own[i][j], other[j][i]
                re = ar * br - ai * bi
                im = ar * bi + ai * br
                real = re if real is None else real + re
                imag = im if imag is None else imag + im
        planes_ref[pl.ds(2 * start, count, stride=2), :] = real
        planes_ref[pl.ds(2 * start + 1, count, stride=2), :] = imag
    lane = lax.broadcasted_iota(jnp.int32, (4, LANES), 1) // 16
    tails = []
    for p in range(6):
        for c in range(2):
            count = 18 if c == 0 else 14
            tiles = planes_ref[pl.ds(36 * p + c, count, stride=2), :]
            msg_ref[0, pl.ds(MSG * 18 * c + p, count, stride=MSG), :] = tiles
        tails.append(planes_ref[pl.ds(36 * p + 28 + 1, 4, stride=2), :])
    for b in range(8):
        packed = jnp.zeros((4, LANES), F32)
        for p in range(6):
            shift = (16 * (p - b)) % LANES
            moved = pltpu.roll(tails[p], shift, 1) if shift else tails[p]
            packed = jnp.where(lane == p, moved, packed)
        msg_ref[0, pl.ds(MSG * b + 6, 4, stride=8 * MSG), :] = packed
    msg_ref[1] = msg_ref[0]


def dot_rows(left, right):
    return lax.dot_general(
        left, right, (((1,), (1,)), ((), ())), preferred_element_type=F32
    )


def correlate_kernel(got_ref, planes_ref, out_ref, result_ref, rows_ref, shift_ref, sem):
    write = pltpu.make_async_copy(planes_ref, result_ref, sem)
    write.start()
    mine = lax.axis_index("zh")

    @pl.when(mine < 2)
    def _():
        correlate(mine, got_ref, out_ref, rows_ref, shift_ref)

    write.wait()


def correlate(mine, got_ref, out_ref, rows_ref, shift_ref):
    lane = lax.broadcasted_iota(jnp.int32, (16, LANES), 1)
    for z in range(4):
        block = (2 * mine + z) % 4
        tails = got_ref[block, pl.ds(6, 16, stride=MSG), :]
        for p in range(6):
            target = pl.ds(96 * z + p, 16, stride=6)
            rows_ref[0, target, :] = got_ref[block, pl.ds(p, 16, stride=MSG), :]
            tail = pltpu.roll(tails, LANES - 16 * p, 1) if p else tails
            rows_ref[1, target, :] = jnp.where(lane < 16, tail, 0.0)
    rows = jnp.concatenate([rows_ref[k] for k in range(2)], axis=1)
    high = rows.astype(jnp.bfloat16)
    low = (rows - high.astype(F32)).astype(jnp.bfloat16)
    both = dot_rows(jnp.concatenate([high[:192], low[:192]], axis=0), high)
    products = both[:192] + (both[192:] + dot_rows(high[:192], low))
    row = lax.broadcasted_iota(jnp.int32, (192, 384), 0)
    for bit in (1, 2, 4):
        products = jnp.where((row & bit) != 0, pltpu.roll(products, 384 - bit, 1), products)
    for g in range(24):
        group = products[8 * g : 8 * g + 8]
        if g:
            group = pltpu.roll(group, 384 - 8 * g, 1)
        for k in range(2):
            shift_ref[k, pl.ds(8 * g, 8), :] = group[:, LANES * k : LANES * (k + 1)]
    lane = lax.broadcasted_iota(jnp.int32, (32, LANES), 1)
    far = []
    for p in range(6):
        out_ref[pl.ds(p, 32, stride=RES), :] = shift_ref[0, pl.ds(p, 32, stride=6), :]
        far.append(shift_ref[1, pl.ds(p, 32, stride=6), :])
    last = jnp.zeros((32, LANES), F32)
    for p in range(6):
        last = jnp.where(lane == p, pltpu.roll(far[p], 64 + p, 1), last)
    out_ref[pl.ds(9, 32, stride=RES), :] = last
    for q in range(3):
        pair = jnp.where(lane < 64, far[2 * q], pltpu.roll(far[2 * q + 1], 64, 1))
        out_ref[pl.ds(6 + q, 32, stride=RES), :] = pair


def total_kernel(pieces_ref, out_ref):
    sums = [
        jnp.sum(pieces_ref[pl.ds(k, 32, stride=RES), :], axis=0, keepdims=True) * (1.0 / 4608.0)
        for k in range(RES)
    ]
    lane = lax.broadcasted_iota(jnp.int32, (1, LANES), 1)
    for p in range(6):
        out_ref[pl.ds(p, 1), pl.ds(0, LANES)] = sums[p]
        far = sums[6 + p // 2]
        far = pltpu.roll(far, 64, 1) if p % 2 else far
        far = jnp.where(lane < 64, far, pltpu.roll(sums[9], 64 - p, 1))
        out_ref[pl.ds(p, 1), pl.ds(LANES, 65)] = far[:, :65]


def vmem(count):
    return [pl.BlockSpec(memory_space=pltpu.VMEM)] * count


def per_device(time_links):
    links = with_layout_constraint(
        time_links.reshape(3, 2, 3, 3, 6, 36, LANES),
        Layout((0, 2, 3, 4, 5, 1, 6)),
    )
    links = jnp.transpose(links, (0, 2, 3, 4, 5, 1, 6)).reshape(3, 3, 3, 432, LANES)
    keep, got = product(links)
    planes, messages = pl.pallas_call(
        trace_kernel,
        in_specs=vmem(2),
        out_specs=vmem(2),
        out_shape=[
            jax.ShapeDtypeStruct((216, LANES), F32),
            jax.ShapeDtypeStruct((2, 32 * MSG, LANES), F32),
        ],
        compiler_params=SMALL,
        name="trace",
    )(keep, got)
    gathered = exchange(messages, ("zh", "zl", "y", "x"), MSG).reshape(4, 16 * MSG, LANES)
    partial, planes = pl.pallas_call(
        correlate_kernel,
        in_specs=vmem(2),
        out_specs=vmem(1) + [pl.BlockSpec(memory_space=pltpu.HBM)],
        out_shape=[
            jax.ShapeDtypeStruct((32 * RES, LANES), F32),
            jax.ShapeDtypeStruct((216, LANES), F32),
        ],
        scratch_shapes=[
            pltpu.VMEM((2, 384, LANES), F32),
            pltpu.VMEM((2, 192, LANES), F32),
            pltpu.SemaphoreType.DMA,
        ],
        compiler_params=SMALL,
        name="correlate",
    )(gathered, planes)
    loop_planes = with_layout_constraint(
        planes.reshape(6, 18, 2, LANES).transpose(0, 2, 1, 3),
        Layout((0, 2, 1, 3)),
    ).reshape(6, 2, 2304)
    partial = partial + lax.ppermute(partial, "ta", [(0, 1), (1, 0)])
    pieces = exchange(partial, ("zl", "y", "x"), RES)
    correlator = pl.pallas_call(
        total_kernel,
        in_specs=vmem(1),
        out_specs=pl.BlockSpec(memory_space=pltpu.VMEM),
        out_shape=jax.ShapeDtypeStruct((6, 193), F32),
        compiler_params=SMALL,
        name="total",
    )(pieces)
    return loop_planes, correlator


def exchange(values, axes, rows):
    shape = values.shape
    tile = 2 - rows % 2
    values = values.reshape(-1, rows // tile, tile, LANES)
    return lax.all_to_all(values, axes, split_axis=0, concat_axis=0, tiled=True).reshape(shape)


def solution(mesh):
    grid = Mesh(mesh.devices.reshape(2, 2, 2, 4, 4), ("ta", "zh", "zl", "y", "x"))
    gx = ("zh", "zl", "y", "x")
    return jax.shard_map(
        per_device,
        mesh=grid,
        in_specs=(P("ta", None, None, None, gx, None),),
        out_specs=(P(gx, None, "ta"), P(gx, None)),
        check_vma=False,
    )
```

```python
import functools

import jax
import jax.numpy as jnp
from jax import lax
from jax.experimental import pallas as pl
from jax.experimental.layout import Layout, with_layout_constraint
from jax.experimental.pallas import tpu as pltpu
from jax.sharding import Mesh, PartitionSpec as P

F32 = jnp.float32
LANES = 128
WIDE = pltpu.CompilerParams(vmem_limit_bytes=50 * 2**20)
SMALL = pltpu.CompilerParams(vmem_limit_bytes=12 * 2**20)


def cross_conj(first, second):
    row = []
    for k in range(3):
        a, b = (k + 1) % 3, (k + 2) % 3
        (fa, ga), (fb, gb) = first[a], first[b]
        (sa, ta), (sb, tb) = second[a], second[b]
        real = (fa * sb - ga * tb) - (fb * sa - gb * ta)
        imag = (fb * ta + gb * sa) - (fa * tb + ga * sb)
        row.append((real, imag))
    return row


def rows_times(rows, matrix):
    out = []
    for row in rows:
        line = []
        for j in range(3):
            real = imag = None
            for m in range(3):
                (ar, ai), (br, bi) = row[m], matrix[m][j]
                re = ar * br - ai * bi
                im = ar * bi + ai * br
                real = re if real is None else real + re
                imag = im if imag is None else imag + im
            line.append((real, imag))
        out.append(line)
    return out


THIRD = 1.0 / 3.0
MSG = 7
RES = 10
CHUNKS = ((0, 8), (8, 8), (16, 2))


def half_reads(half, links_ref, links, sems, planes=range(6)):
    copies = []
    for i, x in enumerate(planes):
        source = pl.ds(pl.multiple_of(72 * x + 32 * half, 8), 40)
        copies.append(
            pltpu.make_async_copy(
                links_ref.at[:, pl.ds(0, 2), :, source, :], links.at[i], sems.at[i]
            )
        )
    return copies


def multiply_half(half, links, out_ref, x, place):
    for start, count in CHUNKS:
        def load(t, i, j):
            return tuple(
                links[place, t, i, j, pl.ds(4 * half + 2 * start + c, count, stride=2), :]
                for c in range(2)
            )

        rows = [[load(0, i, j) for j in range(3)] for i in range(2)]
        for t in (1, 2):
            matrix = [[load(t, i, j) for j in range(3)] for i in range(2)]
            matrix.append(cross_conj(matrix[0], matrix[1]))
            rows = rows_times(rows, matrix)
        if out_ref.shape[0] == 18:
            rows.append(cross_conj(rows[0], rows[1]))
            rows = [[(re * THIRD, im * THIRD) for re, im in row] for row in rows]
        for i, row in enumerate(rows):
            for j in range(3):
                for c in range(2):
                    m = 6 * i + 2 * j + c
                    if len(out_ref.shape) == 2:
                        out_ref[pl.ds(108 * m + 18 * x + start, count), :] = row[j][c]
                    else:
                        out_ref[m, pl.ds(18 * x + start, count), :] = row[j][c]


EARLY = 2


def sent_kernel(links_ref, out_ref, early, links, sems, early_sems):
    mine = lax.axis_index("ta")
    copies = half_reads(1 - mine, links_ref, links, sems)
    ahead = half_reads(mine, links_ref, early, early_sems, range(EARLY))
    for copy in copies + ahead:
        copy.start()
    for x in range(6):
        copies[x].wait()
        multiply_half(1 - mine, links, out_ref, x, x)
    for copy in ahead:
        copy.wait()


def kept_kernel(links_ref, early, out_ref, links, sems):
    mine = lax.axis_index("ta")
    copies = half_reads(mine, links_ref, links, sems, range(EARLY, 6))
    for copy in copies:
        copy.start()
    for x in range(EARLY):
        multiply_half(mine, early, out_ref, x, x)
    for x in range(EARLY, 6):
        copies[x - EARLY].wait()
        multiply_half(mine, links, out_ref, x, x - EARLY)


def product(links):
    hbm = [pl.BlockSpec(memory_space=pltpu.HBM)]
    cost = pl.CostEstimate(flops=40_000_000, bytes_accessed=2_000_000, transcendentals=0)
    sent, early = pl.pallas_call(
        sent_kernel,
        in_specs=hbm,
        out_specs=vmem(2),
        out_shape=[
            jax.ShapeDtypeStruct((1296, LANES), F32),
            jax.ShapeDtypeStruct((EARLY, 3, 2, 3, 40, LANES), F32),
        ],
        scratch_shapes=[
            pltpu.VMEM((6, 3, 2, 3, 40, LANES), F32),
            pltpu.SemaphoreType.DMA((6,)),
            pltpu.SemaphoreType.DMA((EARLY,)),
        ],
        compiler_params=WIDE,
        cost_estimate=cost,
        name="product_sent",
    )(links)
    got = lax.ppermute(sent, "ta", [(0, 1), (1, 0)])
    keep = pl.pallas_call(
        kept_kernel,
        in_specs=hbm + vmem(1),
        out_specs=pl.BlockSpec(memory_space=pltpu.VMEM),
        out_shape=jax.ShapeDtypeStruct((18, 108, LANES), F32),
        scratch_shapes=[
            pltpu.VMEM((6 - EARLY, 3, 2, 3, 40, LANES), F32),
            pltpu.SemaphoreType.DMA((6 - EARLY,)),
        ],
        compiler_params=WIDE,
        cost_estimate=cost,
        name="product_kept",
    )(links, early)
    return keep, got


def trace_kernel(keep_ref, got_ref, planes_ref, msg_ref):
    for start in range(0, 108, 8):
        count = min(8, 108 - start)

        def at(ref, m):
            if len(ref.shape) == 2:
                return ref[pl.ds(108 * m + start, count), :]
            return ref[m, pl.ds(start, count), :]

        def load(ref, rows):
            return [
                [
                    tuple(at(ref, 6 * i + 2 * j + c) for c in range(2))
                    for j in range(3)
                ]
                for i in range(rows)
            ]

        own, other = load(keep_ref, 3), load(got_ref, 2)
        other.append(cross_conj(other[0], other[1]))
        real = imag = None
        for i in range(3):
            for j in range(3):
                (ar, ai), (br, bi) = own[i][j], other[j][i]
                re = ar * br - ai * bi
                im = ar * bi + ai * br
                real = re if real is None else real + re
                imag = im if imag is None else imag + im
        planes_ref[pl.ds(2 * start, count, stride=2), :] = real
        planes_ref[pl.ds(2 * start + 1, count, stride=2), :] = imag
    lane = lax.broadcasted_iota(jnp.int32, (4, LANES), 1) // 16
    tails = []
    for p in range(6):
        for c in range(2):
            count = 18 if c == 0 else 14
            tiles = planes_ref[pl.ds(36 * p + c, count, stride=2), :]
            msg_ref[0, pl.ds(MSG * 18 * c + p, count, stride=MSG), :] = tiles
        tails.append(planes_ref[pl.ds(36 * p + 28 + 1, 4, stride=2), :])
    for b in range(8):
        packed = jnp.zeros((4, LANES), F32)
        for p in range(6):
            shift = (16 * (p - b)) % LANES
            moved = pltpu.roll(tails[p], shift, 1) if shift else tails[p]
            packed = jnp.where(lane == p, moved, packed)
        msg_ref[0, pl.ds(MSG * b + 6, 4, stride=8 * MSG), :] = packed
    msg_ref[1] = msg_ref[0]


def dot_rows(left, right):
    return lax.dot_general(
        left, right, (((1,), (1,)), ((), ())), preferred_element_type=F32
    )


def correlate_kernel(got_ref, planes_ref, out_ref, result_ref, rows_ref, shift_ref, sem):
    write = pltpu.make_async_copy(planes_ref, result_ref, sem)
    write.start()
    mine = lax.axis_index("zh")

    @pl.when(mine < 2)
    def _():
        correlate(mine, got_ref, out_ref, rows_ref, shift_ref)

    write.wait()


def correlate(mine, got_ref, out_ref, rows_ref, shift_ref):
    lane = lax.broadcasted_iota(jnp.int32, (16, LANES), 1)
    for z in range(4):
        block = (2 * mine + z) % 4
        tails = got_ref[block, pl.ds(6, 16, stride=MSG), :]
        for p in range(6):
            target = pl.ds(96 * z + p, 16, stride=6)
            rows_ref[0, target, :] = got_ref[block, pl.ds(p, 16, stride=MSG), :]
            tail = pltpu.roll(tails, LANES - 16 * p, 1) if p else tails
            rows_ref[1, target, :] = jnp.where(lane < 16, tail, 0.0)
    rows = jnp.concatenate([rows_ref[k] for k in range(2)], axis=1)
    high = rows.astype(jnp.bfloat16)
    low = (rows - high.astype(F32)).astype(jnp.bfloat16)
    both = dot_rows(jnp.concatenate([high[:192], low[:192]], axis=0), high)
    products = both[:192] + (both[192:] + dot_rows(high[:192], low))
    row = lax.broadcasted_iota(jnp.int32, (192, 384), 0)
    for bit in (1, 2, 4):
        products = jnp.where((row & bit) != 0, pltpu.roll(products, 384 - bit, 1), products)
    for g in range(24):
        group = products[8 * g : 8 * g + 8]
        if g:
            group = pltpu.roll(group, 384 - 8 * g, 1)
        for k in range(2):
            shift_ref[k, pl.ds(8 * g, 8), :] = group[:, LANES * k : LANES * (k + 1)]
    lane = lax.broadcasted_iota(jnp.int32, (32, LANES), 1)
    far = []
    for p in range(6):
        out_ref[pl.ds(p, 32, stride=RES), :] = shift_ref[0, pl.ds(p, 32, stride=6), :]
        far.append(shift_ref[1, pl.ds(p, 32, stride=6), :])
    last = jnp.zeros((32, LANES), F32)
    for p in range(6):
        last = jnp.where(lane == p, pltpu.roll(far[p], 64 + p, 1), last)
    out_ref[pl.ds(9, 32, stride=RES), :] = last
    for q in range(3):
        pair = jnp.where(lane < 64, far[2 * q], pltpu.roll(far[2 * q + 1], 64, 1))
        out_ref[pl.ds(6 + q, 32, stride=RES), :] = pair


def total_kernel(pieces_ref, out_ref):
    sums = [
        jnp.sum(pieces_ref[pl.ds(k, 32, stride=RES), :], axis=0, keepdims=True) * (1.0 / 4608.0)
        for k in range(RES)
    ]
    lane = lax.broadcasted_iota(jnp.int32, (1, LANES), 1)
    for p in range(6):
        out_ref[pl.ds(p, 1), pl.ds(0, LANES)] = sums[p]
        far = sums[6 + p // 2]
        far = pltpu.roll(far, 64, 1) if p % 2 else far
        far = jnp.where(lane < 64, far, pltpu.roll(sums[9], 64 - p, 1))
        out_ref[pl.ds(p, 1), pl.ds(LANES, 65)] = far[:, :65]


def vmem(count):
    return [pl.BlockSpec(memory_space=pltpu.VMEM)] * count


def per_device(time_links):
    links = with_layout_constraint(
        time_links.reshape(3, 2, 3, 3, 6, 36, LANES),
        Layout((0, 2, 3, 4, 5, 1, 6)),
    )
    links = jnp.transpose(links, (0, 2, 3, 4, 5, 1, 6)).reshape(3, 3, 3, 432, LANES)
    keep, got = product(links)
    planes, messages = pl.pallas_call(
        trace_kernel,
        in_specs=vmem(2),
        out_specs=vmem(2),
        out_shape=[
            jax.ShapeDtypeStruct((216, LANES), F32),
            jax.ShapeDtypeStruct((2, 32 * MSG, LANES), F32),
        ],
        compiler_params=SMALL,
        name="trace",
    )(keep, got)
    gathered = exchange(messages, ("zh", "zl", "y", "x"), MSG).reshape(4, 16 * MSG, LANES)
    partial, planes = pl.pallas_call(
        correlate_kernel,
        in_specs=vmem(2),
        out_specs=vmem(1) + [pl.BlockSpec(memory_space=pltpu.HBM)],
        out_shape=[
            jax.ShapeDtypeStruct((32 * RES, LANES), F32),
            jax.ShapeDtypeStruct((216, LANES), F32),
        ],
        scratch_shapes=[
            pltpu.VMEM((2, 384, LANES), F32),
            pltpu.VMEM((2, 192, LANES), F32),
            pltpu.SemaphoreType.DMA,
        ],
        compiler_params=SMALL,
        name="correlate",
    )(gathered, planes)
    loop_planes = with_layout_constraint(
        planes.reshape(6, 18, 2, LANES).transpose(0, 2, 1, 3),
        Layout((0, 2, 1, 3)),
    ).reshape(6, 2, 2304)
    partial = partial + lax.ppermute(partial, "ta", [(0, 1), (1, 0)])
    pieces = exchange(partial, ("zl", "y", "x"), RES)
    correlator = pl.pallas_call(
        total_kernel,
        in_specs=vmem(1),
        out_specs=pl.BlockSpec(memory_space=pltpu.VMEM),
        out_shape=jax.ShapeDtypeStruct((6, 193), F32),
        compiler_params=SMALL,
        name="total",
    )(pieces)
    return loop_planes, correlator


def exchange(values, axes, rows):
    shape = values.shape
    tile = 2 - rows % 2
    values = values.reshape(-1, rows // tile, tile, LANES)
    return lax.all_to_all(values, axes, split_axis=0, concat_axis=0, tiled=True).reshape(shape)


def solution(mesh):
    grid = Mesh(mesh.devices.reshape(2, 2, 2, 4, 4), ("ta", "zh", "zl", "y", "x"))
    gx = ("zh", "zl", "y", "x")
    return jax.shard_map(
        per_device,
        mesh=grid,
        in_specs=(P("ta", None, None, None, gx, None),),
        out_specs=(P(gx, None, "ta"), P(gx, None)),
        check_vma=False,
    )
```
